16 devices in a mesh: dp: 1, ep: 16 (over x, y, z, core).
Axes of the slice: x: 2, y: 2, z: 2, core: 2. Of those that a mesh axis runs over, the one named last changes fastest.
Arguments:
- x: bfloat16 [1, 16, 256, 3072], P('dp', 'ep')
- expert: int32 [1, 16, 256, 4], P('dp', 'ep')
- slot: int32 [1, 16, 256, 4], P('dp', 'ep')
- gate: float32 [1, 16, 256, 4], P('dp', 'ep')
- w_gate: bfloat16 [16, 3072, 10752], P('ep')
- w_up: bfloat16 [16, 3072, 10752], P('ep')
- w_down: bfloat16 [16, 10752, 3072], P('ep')
Outputs:
- y: bfloat16 [1, 16, 256, 3072], P('dp', 'ep')
All inputs are finite; a program needn't handle non-finite values.
Results may differ from the reference program's by a relative error of at most 0.009.
Values are sent between devices in bfloat16 or wider.
A program may use at most 2 GiB of HBM per device.

```python
import jax
import jax.numpy as jnp

MEMBERS = 16
TOKENS = 256
D = 3072
FF = 10752
TOP = 4
EXPERTS = 16
SLOTS = 5 * TOKENS * TOP // (4 * EXPERTS)


def setup_inputs(seed: int = 0, part: int = 0) -> dict:
    own, k1, k2, k3, k4, k5, k6 = jax.random.split(jax.random.key(seed), 7)
    kx, ke, kl, kg = jax.random.split(jax.random.fold_in(own, part), 4)
    devices = (1, MEMBERS)
    place = jax.random.permutation(kl, jnp.arange(EXPERTS, dtype=jnp.uint32))
    slow = ((EXPERTS + (9 * place) % EXPERTS) << ((9 * place) // EXPERTS)) // EXPERTS
    wait = (jax.random.bits(ke, (*devices, TOKENS, EXPERTS), jnp.uint32) >> 10) * slow
    expert = jnp.argsort(wait, axis=-1)[..., :TOP].astype(jnp.int32)
    chosen = jax.nn.one_hot(expert, EXPERTS, dtype=jnp.int32)
    in_line = jnp.cumsum(chosen.reshape(*devices, TOKENS * TOP, EXPERTS), axis=2) - 1
    slot = jnp.sum(in_line.reshape(chosen.shape) * chosen, axis=-1)

    def one(key, rows, columns):
        return (jax.random.normal(key, (rows, columns), jnp.float32) * rows**-0.5).astype(jnp.bfloat16)

    def weights(key, rows, columns):
        return jax.lax.map(lambda k: one(k, rows, columns), jax.random.split(key, EXPERTS))

    return {
        "x": jax.random.normal(kx, (*devices, TOKENS, D), jnp.float32).astype(jnp.bfloat16),
        "expert": expert,
        "slot": slot,
        "gate": jax.nn.softmax(jax.random.normal(kg, expert.shape, jnp.float32)),
        "w_gate": weights(k1, D, FF),
        "w_up": weights(k2, D, FF),
        "w_down": weights(k3, FF, D),
    }


def einsum(form, a, b):
    return jnp.einsum(form, a.astype(jnp.float32), b.astype(jnp.float32))


def reference(x, expert, slot, gate, w_gate, w_up, w_down):
    to_expert = jax.nn.one_hot(expert, EXPERTS, dtype=jnp.bfloat16)
    to_slot = jax.nn.one_hot(slot, SLOTS, dtype=jnp.bfloat16)
    weighted = to_expert * gate[..., None].astype(jnp.bfloat16)
    dispatch = einsum("abtke,abtkc->abtec", to_expert, to_slot).astype(jnp.bfloat16)
    combine = einsum("abtke,abtkc->abtec", weighted, to_slot).astype(jnp.bfloat16)
    z = einsum("abtec,abtd->aebcd", dispatch, x).astype(jnp.bfloat16)
    h = jax.nn.silu(einsum("aebcd,edf->aebcf", z, w_gate))
    h = (h * einsum("aebcd,edf->aebcf", z, w_up)).astype(jnp.bfloat16)
    out = einsum("aebcf,efd->aebcd", h, w_down).astype(jnp.bfloat16)
    y = einsum("abtec,aebcd->abtd", combine, out)
    return y.astype(jnp.bfloat16)
```

```python
import functools

import jax
import jax.numpy as jnp
from jax import lax
from jax.experimental import pallas as pl
from jax.experimental.pallas import tpu as pltpu
from jax.sharding import PartitionSpec as P

MESH = pl.DeviceIdType.MESH
PASSES = ((0, 1, 8, 4, 2), (12, 10, 6, 13, 11, 7, 14), (9, 5, 3, 15))
ORDER = tuple(k for group in PASSES for k in group)
TF, TN = 512, 256
N1, N2 = 3, 3


def flip(me, k):
    to = me
    for b in range(4):
        if (k >> b) & 1:
            to = to + (1 << b) * (1 - 2 * lax.rem(lax.div(me, 1 << b), 2))
    return to


def kernel(slots, z_in, wg, wu, wd, ret, z, h, w1g, w1u, w2, zsend, zrecv, s1, s2, rsend, rrecv):
    me = lax.axis_index("ep")
    depth, ff = wg.shape
    n_ff, n_d, n_pass = ff // TF, depth // TN, len(PASSES)

    def rows(pos):
        return pl.ds(pos * slots, slots)

    def peer(k):
        return {"ep": flip(me, k)}

    def block_in(pos):
        k = ORDER[pos]
        if k == 0:
            return pltpu.make_async_copy(z_in.at[rows(pos)], z.at[rows(pos)], zrecv.at[pos])
        return pltpu.make_async_remote_copy(
            z_in.at[rows(pos)], z.at[rows(pos)], zsend.at[pos], zrecv.at[pos], device_id=peer(k), device_id_type=MESH
        )

    def block_out(pos, columns=None):
        k = ORDER[pos]
        here = (rows(pos),) if columns is None else (rows(pos), columns)
        if k == 0:
            return pltpu.make_async_copy(z.at[here], ret.at[here], rrecv.at[pos])
        return pltpu.make_async_remote_copy(
            z.at[here], ret.at[here], rsend.at[pos], rrecv.at[pos], device_id=peer(k), device_id_type=MESH
        )

    def up_tiles(i):
        tile, slot = lax.rem(i, n_ff), lax.rem(i, N1)
        columns = pl.ds(pl.multiple_of(tile * TF, TF), TF)
        return (
            pltpu.make_async_copy(wg.at[:, columns], w1g.at[slot], s1.at[0, slot]),
            pltpu.make_async_copy(wu.at[:, columns], w1u.at[slot], s1.at[1, slot]),
        )

    def down_tile(j):
        tile, slot = lax.rem(j, n_d), lax.rem(j, N2)
        columns = pl.ds(pl.multiple_of(tile * TN, TN), TN)
        return pltpu.make_async_copy(wd.at[:, columns], w2.at[slot], s2.at[slot])

    for pos in range(len(ORDER)):
        block_in(pos).start()
    for i in range(N1 - 1):
        for copy in up_tiles(i):
            copy.start()
    for j in range(N2 - 1):
        down_tile(j).start()

    first = 0
    for p, group in enumerate(PASSES):
        last = p == n_pass - 1
        here = range(first, first + len(group))
        start, size = first * slots, len(group) * slots
        for pos in here:
            if ORDER[pos] == 0:
                block_in(pos).wait()
            else:
                block_in(pos).wait_recv()

        def up(t, carry, p=p, start=start, size=size):
            i = p * n_ff + t

            @pl.when(i + N1 - 1 < n_pass * n_ff)
            def _():
                for copy in up_tiles(i + N1 - 1):
                    copy.start()

            for copy in up_tiles(i):
                copy.wait()
            slot = lax.rem(i, N1)
            for n in range(0, TF, 256):
                rhs = z[pl.ds(start, size), :]
                g = jnp.dot(rhs, w1g[slot, :, n : n + 256], preferred_element_type=jnp.float32)
                u = jnp.dot(rhs, w1u[slot, :, n : n + 256], preferred_element_type=jnp.float32)
                columns = pl.ds(pl.multiple_of(t * TF + n, 256), 256)
                h[pl.ds(0, size), columns] = (jax.nn.silu(g) * u).astype(jnp.bfloat16)
            return carry

        lax.fori_loop(0, n_ff, up, 0)

        def down(n, carry, p=p, start=start, size=size, here=here, last=last):
            j = p * n_d + n

            @pl.when(j + N2 - 1 < n_pass * n_d)
            def _():
                down_tile(j + N2 - 1).start()

            if last:

                @pl.when(n > 0)
                def _():
                    for pos in here:
                        block_out(pos, pl.ds(pl.multiple_of((n - 1) * TN, TN), TN)).start()

            down_tile(j).wait()
            slot = lax.rem(j, N2)
            out = jnp.dot(h[pl.ds(0, size), :], w2[slot], preferred_element_type=jnp.float32)
            z[pl.ds(start, size), pl.ds(pl.multiple_of(n * TN, TN), TN)] = out.astype(jnp.bfloat16)
            return carry

        lax.fori_loop(0, n_d, down, 0)
        for pos in here:
            if last:
                block_out(pos, pl.ds((n_d - 1) * TN, TN)).start()
            else:
                block_out(pos).start()
        first += len(group)

    for pos in range(len(ORDER)):
        if ORDER[pos] == 0:
            block_out(pos).wait()
        else:
            block_in(pos).wait_send()
            block_out(pos).wait()


def solution(mesh):
    def step(x, expert, slot, gate, w_gate, w_up, w_down):
        tokens, top = expert.shape[2:]
        depth, ff = w_gate.shape[1:]
        experts = mesh.shape["ep"]
        slots = 5 * tokens * top // (4 * experts)
        held = experts * slots
        me = lax.axis_index("ep")
        x, expert, slot, gate = x[0, 0], expert[0, 0].T, slot[0, 0].T, gate[0, 0].T
        apart = jnp.bitwise_xor(expert, me)
        place = sum(jnp.where(apart == k, pos, 0) for pos, k in enumerate(ORDER))
        row = jnp.where(slot < slots, place * slots + slot, -1)
        at = lax.broadcasted_iota(jnp.int32, (held, tokens), 0)
        hit = [at == row[j][None, :] for j in range(top)]
        dispatch = functools.reduce(jnp.logical_or, hit).astype(jnp.bfloat16)
        weight = gate.astype(jnp.bfloat16).astype(jnp.float32)
        combine = sum(jnp.where(hit[j], weight[j][None, :], 0.0) for j in range(top)).astype(jnp.bfloat16)
        z = jnp.dot(dispatch, x, preferred_element_type=jnp.float32).astype(jnp.bfloat16)
        most = max(len(group) for group in PASSES) * slots
        n = len(ORDER)
        ret = pl.pallas_call(
            functools.partial(kernel, slots),
            out_shape=jax.ShapeDtypeStruct((held, depth), jnp.bfloat16),
            in_specs=[pl.BlockSpec(memory_space=pl.ANY)] * 4,
            out_specs=pl.BlockSpec(memory_space=pl.ANY),
            scratch_shapes=[
                pltpu.VMEM((held, depth), jnp.bfloat16),
                pltpu.VMEM((most, ff), jnp.bfloat16),
                pltpu.VMEM((N1, depth, TF), jnp.bfloat16),
                pltpu.VMEM((N1, depth, TF), jnp.bfloat16),
                pltpu.VMEM((N2, ff, TN), jnp.bfloat16),
                pltpu.SemaphoreType.DMA((n,)),
                pltpu.SemaphoreType.DMA((n,)),
                pltpu.SemaphoreType.DMA((2, N1)),
                pltpu.SemaphoreType.DMA((N2,)),
                pltpu.SemaphoreType.DMA((n,)),
                pltpu.SemaphoreType.DMA((n,)),
            ],
            compiler_params=pltpu.CompilerParams(vmem_limit_bytes=67043328, has_side_effects=True),
        )(z, w_gate[0], w_up[0], w_down[0])
        y = lax.dot_general(combine, ret, (((0,), (0,)), ((), ())), preferred_element_type=jnp.float32)
        return y.astype(jnp.bfloat16)[None, None]

    block = P("dp", "ep", None, None)
    weights = P("ep", None, None)
    return jax.shard_map(
        step, mesh=mesh, in_specs=(block,) * 4 + (weights,) * 3, out_specs=block, check_vma=False
    )
```

```python
import functools

import jax
import jax.numpy as jnp
from jax import lax
from jax.experimental import pallas as pl
from jax.experimental.pallas import tpu as pltpu
from jax.sharding import PartitionSpec as P

MESH = pl.DeviceIdType.MESH
PASSES = ((1, 8, 4, 2), (12, 10, 6, 13, 11, 7, 15), (0, 9, 5, 3, 14))
ORDER = tuple(k for group in PASSES for k in group)
SENDS = ({0: (12, 10, 6), 9: (13, 11, 7), 17: (15,)}, {1: (9, 5, 3), 6: (14,)}, {})
RETURNS = ({}, {0: (1, 8, 4, 2)}, {0: (12, 10, 6), 8: (13, 11, 7), 16: (15,)})
TF, TN = 512, 256
N1, N2 = 3, 3


def flip(me, k):
    to = me
    for b in range(4):
        if (k >> b) & 1:
            to = to + (1 << b) * (1 - 2 * lax.rem(lax.div(me, 1 << b), 2))
    return to


def kernel(slots, x, row, wg, wu, wd, ret, z, h, late, w1g, w1u, w2, zsend, zrecv, s1, s2, rsend, rrecv):
    me = lax.axis_index("ep")
    depth, ff = wg.shape
    n_ff, n_d, n_pass = ff // TF, depth // TN, len(PASSES)
    n_a, n_b = len(PASSES[0]), len(PASSES[1])

    def rows(pos):
        return pl.ds(pos * slots, slots)

    def peer(k):
        return {"ep": flip(me, k)}

    def staged(pos, column=0, width=None):
        width = depth if width is None else width
        if ORDER[pos] == 0:
            return z.at[rows(pos), pl.ds(column, width)]
        if pos < n_a:
            return h.at[rows(pos), pl.ds(column, width)]
        if pos < n_a + n_b:
            at = pos - n_a
            return h.at[rows(n_a + at // 3), pl.ds((at % 3) * depth + column, width)]
        return late.at[rows(pos - n_a - n_b - 1), pl.ds(column, width)]

    def fill(first, count):
        at = lax.broadcasted_iota(jnp.int32, (count * slots, row.shape[1]), 0) + first * slots
        hit = functools.reduce(jnp.logical_or, [at == row[j : j + 1, :] for j in range(row.shape[0])])
        pick = jnp.where(hit, 1.0, 0.0).astype(jnp.bfloat16)
        for column in range(0, depth, 256):
            block = jnp.dot(pick, x[:, column : column + 256], preferred_element_type=jnp.float32)
            block = block.astype(jnp.bfloat16)
            for i in range(count):
                staged(first + i, column, 256)[...] = block[i * slots : (i + 1) * slots]

    def block_in(pos):
        return pltpu.make_async_remote_copy(
            staged(pos), z.at[rows(pos)], zsend.at[pos], zrecv.at[pos], device_id=peer(ORDER[pos]), device_id_type=MESH
        )

    def block_out(pos, columns=None):
        k = ORDER[pos]
        here = (rows(pos),) if columns is None else (rows(pos), columns)
        if k == 0:
            return pltpu.make_async_copy(z.at[here], ret.at[here], rrecv.at[pos])
        return pltpu.make_async_remote_copy(
            z.at[here], ret.at[here], rsend.at[pos], rrecv.at[pos], device_id=peer(k), device_id_type=MESH
        )

    def up_tiles(i):
        tile, slot = lax.rem(i, n_ff), lax.rem(i, N1)
        columns = pl.ds(pl.multiple_of(tile * TF, TF), TF)
        return (
            pltpu.make_async_copy(wg.at[:, columns], w1g.at[slot], s1.at[0, slot]),
            pltpu.make_async_copy(wu.at[:, columns], w1u.at[slot], s1.at[1, slot]),
        )

    def down_tile(j):
        tile, slot = lax.rem(j, n_d), lax.rem(j, N2)
        columns = pl.ds(pl.multiple_of(tile * TN, TN), TN)
        return pltpu.make_async_copy(wd.at[:, columns], w2.at[slot], s2.at[slot])

    for i in range(N1 - 1):
        for copy in up_tiles(i):
            copy.start()
    for j in range(N2 - 1):
        down_tile(j).start()
    fill(0, n_a)
    for pos in range(n_a):
        block_in(pos).start()
    fill(n_a, n_b)
    fill(n_a + n_b, len(ORDER) - n_a - n_b)

    first = 0
    for p, group in enumerate(PASSES):
        last = p == n_pass - 1
        here = range(first, first + len(group))
        start, size = first * slots, len(group) * slots
        for pos in here:
            if ORDER[pos] != 0:
                block_in(pos).wait_recv()
                if not last:
                    block_in(pos).wait_send()

        def up(t, carry, p=p, start=start, size=size):
            i = p * n_ff + t

            @pl.when(i + N1 - 1 < n_pass * n_ff)
            def _():
                for copy in up_tiles(i + N1 - 1):
                    copy.start()

            for copy in up_tiles(i):
                copy.wait()
            for at, blocks in SENDS[p].items():

                @pl.when(t == at)
                def _(blocks=blocks):
                    for k in blocks:
                        block_in(ORDER.index(k)).start()

            for at, blocks in RETURNS[p].items():

                @pl.when(t == at)
                def _(blocks=blocks):
                    for k in blocks:
                        block_out(ORDER.index(k)).start()

            slot = lax.rem(i, N1)
            for n in range(0, TF, 256):
                rhs = z[pl.ds(start, size), :]
                g = jnp.dot(rhs, w1g[slot, :, n : n + 256], preferred_element_type=jnp.float32)
                u = jnp.dot(rhs, w1u[slot, :, n : n + 256], preferred_element_type=jnp.float32)
                columns = pl.ds(pl.multiple_of(t * TF + n, 256), 256)
                h[pl.ds(0, size), columns] = (jax.nn.silu(g) * u).astype(jnp.bfloat16)
            return carry

        lax.fori_loop(0, n_ff, up, 0)

        def down(n, carry, p=p, start=start, size=size, here=here, last=last):
            j = p * n_d + n

            @pl.when(j + N2 - 1 < n_pass * n_d)
            def _():
                down_tile(j + N2 - 1).start()

            if last:

                @pl.when(n > 0)
                def _():
                    for pos in here:
                        block_out(pos, pl.ds(pl.multiple_of((n - 1) * TN, TN), TN)).start()

            down_tile(j).wait()
            slot = lax.rem(j, N2)
            out = jnp.dot(h[pl.ds(0, size), :], w2[slot], preferred_element_type=jnp.float32)
            z[pl.ds(start, size), pl.ds(pl.multiple_of(n * TN, TN), TN)] = out.astype(jnp.bfloat16)
            return carry

        lax.fori_loop(0, n_d, down, 0)
        if last:
            for pos in here:
                block_out(pos, pl.ds((n_d - 1) * TN, TN)).start()
        first += len(group)

    for pos in range(len(ORDER)):
        if ORDER[pos] == 0:
            block_out(pos).wait()
        else:
            if pos >= n_a + n_b:
                block_in(pos).wait_send()
            block_out(pos).wait()


def solution(mesh):
    def step(x, expert, slot, gate, w_gate, w_up, w_down):
        tokens, top = expert.shape[2:]
        depth, ff = w_gate.shape[1:]
        experts = mesh.shape["ep"]
        slots = 5 * tokens * top // (4 * experts)
        held = experts * slots
        me = lax.axis_index("ep")
        x, expert, slot, gate = x[0, 0], expert[0, 0].T, slot[0, 0].T, gate[0, 0].T
        apart = jnp.bitwise_xor(expert, me)
        place = sum(jnp.where(apart == k, pos, 0) for pos, k in enumerate(ORDER))
        row = jnp.where(slot < slots, place * slots + slot, -1)
        at = lax.broadcasted_iota(jnp.int32, (held, tokens), 0)
        hit = [at == row[j][None, :] for j in range(top)]
        weight = gate.astype(jnp.bfloat16).astype(jnp.float32)
        combine = sum(jnp.where(hit[j], weight[j][None, :], 0.0) for j in range(top)).astype(jnp.bfloat16)
        most = max(len(group) for group in PASSES) * slots
        n = len(ORDER)
        ret = pl.pallas_call(
            functools.partial(kernel, slots),
            out_shape=jax.ShapeDtypeStruct((held, depth), jnp.bfloat16),
            in_specs=[pl.BlockSpec(memory_space=pltpu.VMEM)] * 2 + [pl.BlockSpec(memory_space=pl.ANY)] * 3,
            out_specs=pl.BlockSpec(memory_space=pl.ANY),
            scratch_shapes=[
                pltpu.VMEM((held, depth), jnp.bfloat16),
                pltpu.VMEM((most, ff), jnp.bfloat16),
                pltpu.VMEM(((len(PASSES[-1]) - 1) * slots, depth), jnp.bfloat16),
                pltpu.VMEM((N1, depth, TF), jnp.bfloat16),
                pltpu.VMEM((N1, depth, TF), jnp.bfloat16),
                pltpu.VMEM((N2, ff, TN), jnp.bfloat16),
                pltpu.SemaphoreType.DMA((n,)),
                pltpu.SemaphoreType.DMA((n,)),
                pltpu.SemaphoreType.DMA((2, N1)),
                pltpu.SemaphoreType.DMA((N2,)),
                pltpu.SemaphoreType.DMA((n,)),
                pltpu.SemaphoreType.DMA((n,)),
            ],
            compiler_params=pltpu.CompilerParams(vmem_limit_bytes=67043328, has_side_effects=True),
        )(x, row, w_gate[0], w_up[0], w_down[0])
        y = lax.dot_general(combine, ret, (((0,), (0,)), ((), ())), preferred_element_type=jnp.float32)
        return y.astype(jnp.bfloat16)[None, None]

    block = P("dp", "ep", None, None)
    weights = P("ep", None, None)
    return jax.shard_map(
        step, mesh=mesh, in_specs=(block,) * 4 + (weights,) * 3, out_specs=block, check_vma=False
    )
```

```python
import functools

import jax
import jax.numpy as jnp
from jax import lax
from jax.experimental import pallas as pl
from jax.experimental.pallas import tpu as pltpu
from jax.sharding import PartitionSpec as P

MESH = pl.DeviceIdType.MESH
SLOTS, CUT = 80, 48
PASSES = (
    ((0, 0, SLOTS), (1, 0, SLOTS), (8, 0, CUT), (4, 0, CUT), (2, 0, CUT)),
    tuple((k, 0, SLOTS) for k in (12, 10, 6, 14, 15)) + tuple((k, CUT, SLOTS) for k in (8, 4, 2)),
    tuple((k, 0, SLOTS) for k in (9, 5, 3, 13, 11, 7)),
)
PIECES = tuple(piece for group in PASSES for piece in group)
SIZES = tuple(stop - start for _, start, stop in PIECES)
STARTS = tuple(sum(SIZES[:i]) for i in range(len(PIECES)))
TF, TN = 512, 256
N1, N2 = 3, 3


def flip(me, k):
    to = me
    for b in range(4):
        if (k >> b) & 1:
            to = to + (1 << b) * (1 - 2 * lax.rem(lax.div(me, 1 << b), 2))
    return to


def kernel(x, row, gate, wg, wu, wd, ret, weights, z, h, late, pick, w1g, w1u, w2, zsend, zrecv, s1, s2, rsend, rrecv, s3):
    me = lax.axis_index("ep")
    depth, ff = wg.shape
    n_ff, n_d, n_pass = ff // TF, depth // TN, len(PASSES)
    n_a, n_b = len(PASSES[0]), len(PASSES[1])
    row_b, row_c = STARTS[n_a], STARTS[n_a + n_b]

    def rows(pos):
        return pl.ds(STARTS[pos], SIZES[pos])

    def peer(k):
        return {"ep": flip(me, k)}

    def staged(pos, column=0, width=None):
        width = depth if width is None else width
        if PIECES[pos][0] == 0:
            return z.at[rows(pos), pl.ds(column, width)]
        if pos < n_a:
            return h.at[rows(pos), pl.ds(column, width)]
        if pos < n_a + n_b:
            whole = sum(size == SLOTS for size in SIZES[n_a : n_a + n_b])
            at = pos - n_a
            first = row_b + at // 3 * SLOTS if at < whole else row_b + -(-whole // 3) * SLOTS
            column += (at if at < whole else at - whole) % 3 * depth
            return h.at[pl.ds(first, SIZES[pos]), pl.ds(column, width)]
        return late.at[pl.ds(STARTS[pos] - row_c, SIZES[pos]), pl.ds(column, width)]

    def hits(first, count):
        at = lax.broadcasted_iota(jnp.int32, (count, row.shape[1]), 0) + first
        return [at == row[j : j + 1, :] for j in range(row.shape[0])]

    def fill(first, count):
        top, total = STARTS[first], sum(SIZES[first : first + count])
        chosen = jnp.where(functools.reduce(jnp.logical_or, hits(top, total)), 1.0, 0.0).astype(jnp.bfloat16)
        for column in range(0, depth, 256):
            block = jnp.dot(chosen, x[:, column : column + 256], preferred_element_type=jnp.float32)
            block = block.astype(jnp.bfloat16)
            for pos in range(first, first + count):
                staged(pos, column, 256)[...] = block[STARTS[pos] - top : STARTS[pos] - top + SIZES[pos]]

    def block_in(pos):
        return pltpu.make_async_remote_copy(
            staged(pos), z.at[rows(pos)], zsend.at[pos], zrecv.at[pos], device_id=peer(PIECES[pos][0]), device_id_type=MESH
        )

    def block_out(pos, columns=None):
        k = PIECES[pos][0]
        here = (rows(pos),) if columns is None else (rows(pos), columns)
        if k == 0:
            return pltpu.make_async_copy(z.at[here], ret.at[here], rrecv.at[pos])
        return pltpu.make_async_remote_copy(
            z.at[here], ret.at[here], rsend.at[pos], rrecv.at[pos], device_id=peer(k), device_id_type=MESH
        )

    def up_tiles(i):
        tile, slot = lax.rem(i, n_ff), lax.rem(i, N1)
        columns = pl.ds(pl.multiple_of(tile * TF, TF), TF)
        return (
            pltpu.make_async_copy(wg.at[:, columns], w1g.at[slot], s1.at[0, slot]),
            pltpu.make_async_copy(wu.at[:, columns], w1u.at[slot], s1.at[1, slot]),
        )

    def down_tile(j):
        tile, slot = lax.rem(j, n_d), lax.rem(j, N2)
        columns = pl.ds(pl.multiple_of(tile * TN, TN), TN)
        return pltpu.make_async_copy(wd.at[:, columns], w2.at[slot], s2.at[slot])

    for i in range(N1 - 1):
        for copy in up_tiles(i):
            copy.start()
    for j in range(N2 - 1):
        down_tile(j).start()
    fill(0, n_a)
    for pos in range(n_a):
        if PIECES[pos][0] != 0:
            block_in(pos).start()
    fill(n_a, n_b)
    fill(n_a + n_b, len(PIECES) - n_a - n_b)
    half = z.shape[0] // 2
    for top in (0, half):
        weight = sum(jnp.where(hit, gate[j : j + 1, :], 0.0) for j, hit in enumerate(hits(top, half)))
        pick[:, pl.ds(top, half)] = weight.T.astype(jnp.bfloat16)
    combine = pltpu.make_async_copy(pick, weights, s3)
    combine.start()

    first, before = 0, ()
    for p, group in enumerate(PASSES):
        last = p == n_pass - 1
        here = range(first, first + len(group))
        start, size = STARTS[first], sum(SIZES[first : first + len(group)])
        for pos in here:
            if PIECES[pos][0] != 0:
                block_in(pos).wait_recv()
                if not last:
                    block_in(pos).wait_send()

        if p == 0:
            for pos in range(n_a, len(PIECES)):
                if PIECES[pos][0] != 0:
                    block_in(pos).start()
        else:
            for pos in before:
                block_out(pos).start()
        before = here

        def up(t, carry, p=p, start=start, size=size):
            i = p * n_ff + t

            @pl.when(i + N1 - 1 < n_pass * n_ff)
            def _():
                for copy in up_tiles(i + N1 - 1):
                    copy.start()

            for copy in up_tiles(i):
                copy.wait()
            slot = lax.rem(i, N1)
            for n in range(0, TF, 256):
                rhs = z[pl.ds(start, size), :]
                g = jnp.dot(rhs, w1g[slot, :, n : n + 256], preferred_element_type=jnp.float32)
                u = jnp.dot(rhs, w1u[slot, :, n : n + 256], preferred_element_type=jnp.float32)
                columns = pl.ds(pl.multiple_of(t * TF + n, 256), 256)
                h[pl.ds(0, size), columns] = (jax.nn.silu(g) * u).astype(jnp.bfloat16)
            return carry

        lax.fori_loop(0, n_ff, up, 0)

        def down(n, carry, p=p, start=start, size=size, here=here, last=last):
            j = p * n_d + n

            @pl.when(j + N2 - 1 < n_pass * n_d)
            def _():
                down_tile(j + N2 - 1).start()

            if last:

                @pl.when(n > 0)
                def _():
                    for pos in here:
                        block_out(pos, pl.ds(pl.multiple_of((n - 1) * TN, TN), TN)).start()

            down_tile(j).wait()
            slot = lax.rem(j, N2)
            out = jnp.dot(h[pl.ds(0, size), :], w2[slot], preferred_element_type=jnp.float32)
            z[pl.ds(start, size), pl.ds(pl.multiple_of(n * TN, TN), TN)] = out.astype(jnp.bfloat16)
            return carry

        lax.fori_loop(0, n_d, down, 0)
        if last:
            for pos in here:
                block_out(pos, pl.ds((n_d - 1) * TN, TN)).start()
        first += len(group)

    combine.wait()
    for pos in range(len(PIECES)):
        if PIECES[pos][0] == 0:
            block_out(pos).wait()
        else:
            if pos >= n_a + n_b:
                block_in(pos).wait_send()
            block_out(pos).wait()


def add_up(combine, ret, y):
    y[...] = jnp.dot(combine[...], ret[...], preferred_element_type=jnp.float32).astype(y.dtype)


def solution(mesh):
    def step(x, expert, slot, gate, w_gate, w_up, w_down):
        tokens, top = expert.shape[2:]
        depth, ff = w_gate.shape[1:]
        experts = mesh.shape["ep"]
        slots = 5 * tokens * top // (4 * experts)
        held = experts * slots
        me = lax.axis_index("ep")
        x, expert, slot, gate = x[0, 0], expert[0, 0].T, slot[0, 0].T, gate[0, 0].T
        apart = jnp.bitwise_xor(expert, me)
        row = jnp.full(slot.shape, -1, jnp.int32)
        for (k, start, stop), first in zip(PIECES, STARTS):
            row = jnp.where((apart == k) & (slot >= start) & (slot < stop), slot - start + first, row)
        weight = gate.astype(jnp.bfloat16).astype(jnp.float32)
        assert slots == SLOTS and held == sum(SIZES)
        most = max(sum(stop - start for _, start, stop in group) for group in PASSES)
        n = len(PIECES)
        ret, combine = pl.pallas_call(
            kernel,
            out_shape=(
                jax.ShapeDtypeStruct((held, depth), jnp.bfloat16),
                jax.ShapeDtypeStruct((tokens, held), jnp.bfloat16),
            ),
            in_specs=[pl.BlockSpec(memory_space=pltpu.VMEM)] * 3 + [pl.BlockSpec(memory_space=pl.ANY)] * 3,
            out_specs=(pl.BlockSpec(memory_space=pl.ANY),) * 2,
            scratch_shapes=[
                pltpu.VMEM((held, depth), jnp.bfloat16),
                pltpu.VMEM((most, ff), jnp.bfloat16),
                pltpu.VMEM((held - STARTS[n - len(PASSES[-1])], depth), jnp.bfloat16),
                pltpu.VMEM((tokens, held), jnp.bfloat16),
                pltpu.VMEM((N1, depth, TF), jnp.bfloat16),
                pltpu.VMEM((N1, depth, TF), jnp.bfloat16),
                pltpu.VMEM((N2, ff, TN), jnp.bfloat16),
                pltpu.SemaphoreType.DMA((n,)),
                pltpu.SemaphoreType.DMA((n,)),
                pltpu.SemaphoreType.DMA((2, N1)),
                pltpu.SemaphoreType.DMA((N2,)),
                pltpu.SemaphoreType.DMA((n,)),
                pltpu.SemaphoreType.DMA((n,)),
                pltpu.SemaphoreType.DMA,
            ],
            compiler_params=pltpu.CompilerParams(vmem_limit_bytes=67043328, has_side_effects=True),
        )(x, row, weight, w_gate[0], w_up[0], w_down[0])
        width = depth // 4
        y = pl.pallas_call(
            add_up,
            out_shape=jax.ShapeDtypeStruct((tokens, depth), jnp.bfloat16),
            grid=(depth // width,),
            in_specs=[pl.BlockSpec((tokens, held), lambda n: (0, 0)), pl.BlockSpec((held, width), lambda n: (0, n))],
            out_specs=pl.BlockSpec((tokens, width), lambda n: (0, n)),
        )(combine, ret)
        return y[None, None]

    block = P("dp", "ep", None, None)
    weights = P("ep", None, None)
    return jax.shard_map(
        step, mesh=mesh, in_specs=(block,) * 4 + (weights,) * 3, out_specs=block, check_vma=False
    )
```
